32 devices in a mesh: grp: 2 (over x), pool: 16 (over z, y, core).
Axes of the slice: x: 2, y: 2, z: 4, core: 2. Of those that a mesh axis runs over, the one named last changes fastest.
Arguments:
- query: bfloat16 [32, 4096], P(('grp', 'pool')), parts along dimension 0, may hold values from -6 to 6
- kv_pool: bfloat16 [2048, 2, 16, 512], P(('grp', 'pool')), parts along dimension 0, may hold values from -6 to 6
- holder_table: int32 [32, 128], P(('grp', 'pool')), parts along dimension 0, may hold values from 0 to 15, as said below
- slot_table: int32 [32, 128], P(('grp', 'pool')), parts along dimension 0, may hold values from 0 to 63
- lengths: int32 [32], P(('grp', 'pool')), parts along dimension 0, may hold values from 96 to 128, as said below
- out_weight: bfloat16 [4096, 8192], P('pool'), may hold values from -1.1953125 to 1.1953125
Outputs:
- mixed: bfloat16 [32, 8192], P(('grp', 'pool')), parts along dimension 0
The draws below stay inside these ranges and needn't reach their ends.
There are 2 independent parts, one for each index of `grp`. The reference program is written for one: setup_inputs(seed, part) draws one part's arguments, and reference() takes and returns one part's arrays. A program takes and returns all parts, laid end to end along the dimension named above; an argument that names none is the same for every part. Nothing has to cross between parts.
Inputs may be any that keep to these rules, and one draw needn't show every extreme that they name: `holder_table`: entry [r, j] is the index along pool of the device holding block j of request r. Of one request's 128 blocks at most 16 have the same holder, and some holder has exactly 16 of the request's first 96 blocks. Request r's live blocks are 0 to lengths[r] - 1; some request has 128.
All inputs are finite; a program needn't handle non-finite values.
Results may differ from the reference program's by a relative error of at most 0.0053.
Values may be sent and summed in bfloat16 or wider, within the bound.
A program may use at most 64 MiB of HBM per device.

```python
import math
import jax
import jax.numpy as jnp
from jax import lax

H = 32
KVH = 4
HD = 128
D = 8192
BLK = 16
MAXB = 128
MINB = 96
SLOTS_DEV = 64
REQUESTS = 16
CAP = 16
N_POOL = 16


def draw_query(key, part):
    groups = H // KVH
    result = jnp.clip(jax.random.normal(jax.random.fold_in(key, 11), (REQUESTS, KVH, groups, HD), jnp.float32), -6.0, 6.0)
    return result.reshape(REQUESTS, H * HD).astype(jnp.bfloat16)


def draw_kv_pool(key, part):
    slot_total = N_POOL * SLOTS_DEV
    result = jnp.clip(jax.random.normal(jax.random.fold_in(key, 21), (slot_total, 2, BLK, KVH, HD), jnp.float32), -6.0, 6.0)
    return result.reshape(slot_total, 2, BLK, KVH * HD).astype(jnp.bfloat16)


def draw_holder_table(key, part):
    spare = (N_POOL - 1) * CAP

    def one_request(request_key):
        home = jax.random.randint(jax.random.fold_in(request_key, 1), (), 0, N_POOL)
        spread = jnp.arange(spare, dtype=jnp.int32)
        others = (home + 1 + spread // CAP) % N_POOL
        order = jax.random.permutation(jax.random.fold_in(request_key, 2), spare)
        picked = others[order][:MAXB - CAP]
        combined = jnp.concatenate([jnp.zeros((CAP,), jnp.int32) + home, picked])
        head_order = jax.random.permutation(jax.random.fold_in(request_key, 3), MINB)
        tail_order = jax.random.permutation(jax.random.fold_in(request_key, 4), MAXB - MINB)
        return jnp.concatenate([combined[:MINB][head_order], combined[MINB:][tail_order]]).astype(jnp.int32)
    return jax.vmap(one_request)(jax.random.split(jax.random.fold_in(key, 31), REQUESTS))


def draw_lengths(key, part):
    result = jax.random.randint(jax.random.fold_in(key, 41), (REQUESTS,), MINB, MAXB + 1)
    longest = jax.random.randint(jax.random.fold_in(key, 43), (), 0, REQUESTS)
    return jnp.where(jnp.arange(REQUESTS, dtype=jnp.int32) == longest, MAXB, result).astype(jnp.int32)


def with_ends(values, rng, smallest, top_value):
    longest = values.shape.index(max(values.shape))
    spots = []
    for shift in (0, 1):
        where = [jax.random.randint(jax.random.fold_in(rng, axis), (), 0, length) for axis, length in enumerate(values.shape)]
        where[longest] = (where[longest] + shift) % values.shape[longest]
        spots.append(tuple(where))
    return values.at[spots[0]].set(smallest).at[spots[1]].set(top_value)


def strengthened(array, key, source, target, shards_of, factor):
    owner, partner = [(jnp.arange(array.shape[position]) // (array.shape[position] // shards_of)).reshape([-1 if axis == position else 1 for axis in range(array.ndim)]) for position in (source, target)]
    chosen = jax.random.permutation(key, shards_of)[partner]
    strong = (owner == chosen) | (owner == (partner + shards_of // 2) % shards_of)
    return jnp.where(strong, factor * array, array)


def levels(key, shape, pieces, least, top_value):
    def one(dim, shards_of):
        heights = jax.random.uniform(jax.random.fold_in(jax.random.fold_in(key, 6), dim), (shards_of,), jnp.float32, least / len(pieces), top_value / len(pieces))
        return jnp.repeat(jnp.exp(heights), shape[dim] // shards_of).reshape((-1,) + (1,) * (len(shape) - dim - 1))

    loudness = one(*pieces[0])
    for cut in pieces[1:]:
        loudness = loudness * one(*cut)
    return loudness


def heavy_noise(rng, extent, scale, bound, pieces, heavy, kind=jnp.bfloat16):
    array = scale * jax.random.normal(rng, extent, jnp.float32)
    if pieces:
        array = array * levels(rng, extent, pieces, -0.22, 0.18)
    return jnp.clip(strengthened(array, jax.random.fold_in(rng, 3), *heavy), -bound, bound).astype(kind)


def setup_inputs(seed: int = 0, part: int = 0) -> dict:
    keys = jax.random.split(jax.random.key(seed), 7)
    part_splits = jax.random.split(jax.random.fold_in(keys[6], part), 7)
    query = draw_query(jax.random.fold_in(jax.random.fold_in(keys[6], part), 71), part)
    kv_pool = draw_kv_pool(jax.random.fold_in(jax.random.fold_in(keys[6], part), 71), part)
    holder_table = draw_holder_table(jax.random.fold_in(jax.random.fold_in(keys[6], part), 71), part)
    slot_table = with_ends(jax.random.randint(part_splits[3], (REQUESTS, MAXB), 0, SLOTS_DEV), jax.random.fold_in(part_splits[3], 1), 0, SLOTS_DEV - 1).astype(jnp.int32)
    lengths = draw_lengths(jax.random.fold_in(jax.random.fold_in(keys[6], part), 71), part)
    out_weight = heavy_noise(keys[5], (H * HD, D), 0.2, 1.1953125, ((0, 16),), (0, 1, 16, 2.0))
    return dict(query=query, kv_pool=kv_pool, holder_table=holder_table, slot_table=slot_table, lengths=lengths, out_weight=out_weight)


lowest = -1e+30

def request_attention(query_heads, block_keys, block_values, live_blocks):
    scores = jnp.einsum('gqd,jbgd->jgqb', query_heads.astype(jnp.float32), block_keys.astype(jnp.float32))
    scores = scores * (1.0 / math.sqrt(HD))
    maxima = lax.optimization_barrier(jnp.max(scores, axis=-1))
    shifted = jnp.exp(scores - maxima[..., None])
    totals = lax.optimization_barrier(jnp.sum(shifted, axis=-1))
    rounded = lax.optimization_barrier(shifted.astype(jnp.bfloat16))
    outputs = jnp.einsum('jgqb,jbgd->jgqd', rounded.astype(jnp.float32), block_values.astype(jnp.float32))
    live_wide = live_blocks[:, None, None]
    peak_score = lax.optimization_barrier(jnp.max(jnp.where(live_wide, maxima, lowest), axis=0))
    factor = jnp.exp(jnp.where(live_wide, maxima - peak_score[None], lowest))
    numerator = lax.optimization_barrier(jnp.sum(factor[..., None] * outputs, axis=0))
    denominator = lax.optimization_barrier(jnp.sum(factor * totals, axis=0))
    return numerator / denominator[..., None]

def reference(query, kv_pool, holder_table, slot_table, lengths, out_weight):

    def one_request(inputs):
        query_row, holders, slot_ids, length = inputs
        pool_rows = holders * SLOTS_DEV + slot_ids
        blocks = kv_pool[pool_rows]
        block_keys = blocks[:, 0].reshape(MAXB, BLK, KVH, HD)
        block_values = blocks[:, 1].reshape(MAXB, BLK, KVH, HD)
        live_blocks = jnp.arange(MAXB, dtype=jnp.int32) < length
        result = request_attention(query_row.reshape(KVH, H // KVH, HD), block_keys, block_values, live_blocks)
        return result.reshape(H * HD).astype(jnp.bfloat16)
    attention = lax.map(one_request, (query, holder_table, slot_table, lengths))
    return jnp.dot(attention, out_weight, preferred_element_type=jnp.float32).astype(jnp.bfloat16)
```

```python
import functools
import math

import jax
import jax.numpy as jnp
from jax import lax
from jax.experimental import pallas as pl
from jax.experimental.pallas import tpu as pltpu
from jax.sharding import PartitionSpec as P

H = 32
KVH = 4
HD = 128
GRP = H // KVH
LOW = -float(2**100)
PAD_A = 8
PAD_B = 16
F32 = jnp.float32
BF16 = jnp.bfloat16


def far_first(n):
    return sorted(range(1, n), key=lambda k: abs(k - n // 2))


def kernel(
    n, slots, blk, hpd,
    len_ref, q_ref, hold_ref, slot_ref, kv_ref, w_ref,
    out_ref,
    stage, msg_a, got_a, qf, expand, kvbuf, wbuf, send_b, got_b, wgt, feat, acc, send_d, got_d,
    sem_as, sem_ar, sem_bs, sem_br, sem_ds, sem_dr, sem_loc, sem_pair_s, sem_pair_r, sem_fs, sem_fr,
):
    me = lax.axis_index("pool")
    core = lax.rem(me, 2)
    chip = me // 2
    partner = me + 1 - 2 * core
    half_heads = H // 2
    half_feat = (KVH // 2) * HD
    half_cols = w_ref.shape[1] // 2
    rows_dev = w_ref.shape[0]
    order = far_first(n)
    rows_a = half_heads + PAD_A

    def at(src, dst, ssem, rsem, peer):
        return pltpu.make_async_remote_copy(
            src_ref=src, dst_ref=dst, send_sem=ssem, recv_sem=rsem,
            device_id={"pool": peer}, device_id_type=pl.DeviceIdType.MESH,
        )

    own_feat = pl.ds(pl.multiple_of(core * half_feat, HD), half_feat)
    other_feat = pl.ds(pl.multiple_of((1 - core) * half_feat, HD), half_feat)
    own_cols = pl.ds(pl.multiple_of(core * half_cols, HD), half_cols)
    other_cols = pl.ds(pl.multiple_of((1 - core) * half_cols, HD), half_cols)
    kv_local = pltpu.make_async_copy(kv_ref.at[:, :, :, own_feat], kvbuf.at[core], sem_loc.at[0])
    w_local = pltpu.make_async_copy(w_ref.at[:, own_cols], wbuf.at[core], sem_loc.at[1])
    kv_local.start()
    w_local.start()

    barrier = pltpu.get_barrier_semaphore()
    for k in order:
        pl.semaphore_signal(
            barrier, inc=1, device_id={"pool": lax.rem(me + k, n)},
            device_id_type=pl.DeviceIdType.MESH,
        )

    maxb = hold_ref.shape[1]
    live = lax.broadcasted_iota(jnp.int32, (1, maxb), 1) < len_ref[0]
    holders = jnp.where(live, hold_ref[...], -1).astype(F32)
    slot_row = slot_ref[...].astype(F32)
    for part in range(2):
        for h in range(half_heads):
            head = part * half_heads + h
            stage[part, h : h + 1, :] = q_ref[:, head * HD : (head + 1) * HD].astype(F32)
        stage[part, half_heads : half_heads + PAD_A, :] = jnp.zeros((PAD_A, HD), F32)
        stage[part, half_heads : half_heads + 1, :] = holders
        stage[part, half_heads + 1 : half_heads + 2, :] = slot_row
    msg_a[...] = stage[...].astype(BF16)

    pl.semaphore_wait(barrier, n - 1)

    sends_a = []
    for k in order:
        peer = lax.rem(me + k, n)
        copy = at(msg_a.at[lax.rem(peer, 2)], got_a.at[me], sem_as.at[k], sem_ar.at[me], peer)
        copy.start()
        sends_a.append(copy)
    kv_pair = at(kv_ref.at[:, :, :, other_feat], kvbuf.at[core], sem_pair_s.at[0], sem_pair_r.at[0], partner)
    kv_pair.start()
    w_pair = at(w_ref.at[:, other_cols], wbuf.at[core], sem_pair_s.at[1], sem_pair_r.at[1], partner)
    w_pair.start()

    slot_pos = lax.broadcasted_iota(jnp.int32, expand.shape, 0)
    token_pos = lax.broadcasted_iota(jnp.int32, expand.shape, 1)
    expand[...] = jnp.where(token_pos // blk == slot_pos, 1.0, 0.0).astype(BF16)

    got_a[me] = msg_a[core]
    for k in reversed(order):
        src = lax.rem(me + n - k, n)
        at(msg_a.at[0], got_a.at[src], sem_as.at[k], sem_ar.at[src], src).wait_recv()
    for r in range(n):
        qf[r * rows_a : (r + 1) * rows_a, :] = got_a[r].astype(F32)

    rel = qf[pl.ds(half_heads, n, stride=rows_a), :].astype(jnp.int32) - 2 * chip
    slot_of = qf[pl.ds(half_heads + 1, n, stride=rows_a), :].astype(jnp.int32)
    code = jnp.where((rel == 0) | (rel == 1), rel * slots + slot_of, -1)
    lane = lax.broadcasted_iota(jnp.int32, (n, 2 * slots), 1)
    count = jnp.zeros((n, 2 * slots), F32)
    for j in range(maxb):
        count += jnp.where(code[:, j : j + 1] == lane, 1.0, 0.0)
    times = jnp.dot(count.astype(BF16), expand[...], preferred_element_type=F32)

    kv_local.wait()
    kv_pair.wait_recv()

    tokens = slots * blk
    scale = 1.0 / math.sqrt(HD)
    dests = n // 2
    per_group = GRP // hpd
    chunk = hpd * n
    lane_sq = lax.broadcasted_iota(jnp.int32, (GRP * n, HD), 1)
    for g in range(KVH // 2):
        cols = slice(g * HD, (g + 1) * HD)
        heads = jnp.concatenate(
            [qf[pl.ds(g * GRP + q, n, stride=rows_a), :] for q in range(GRP)], axis=0
        ).astype(BF16)
        scores = []
        for d in range(2):
            keys = kvbuf[d, :, 0, :, cols].reshape(tokens, HD)
            s = lax.dot_general(heads, keys, (((1,), (1,)), ((), ())), preferred_element_type=F32)
            s = (s * scale).reshape(GRP, n, tokens)
            here = times[:, d * tokens : (d + 1) * tokens]
            scores.append(jnp.where((here > 0.0)[None], s, LOW))
        peak = jnp.maximum(
            jnp.max(scores[0], axis=-1, keepdims=True), jnp.max(scores[1], axis=-1, keepdims=True)
        )
        peak = peak.astype(BF16).astype(F32)
        total = jnp.zeros((GRP, n, 1), F32)
        numer = jnp.zeros((GRP * n, HD), F32)
        for d in range(2):
            here = times[:, d * tokens : (d + 1) * tokens]
            p = jnp.exp(scores[d] - peak) * here[None]
            total += jnp.sum(p, axis=-1, keepdims=True)
            values = kvbuf[d, :, 1, :, cols].reshape(tokens, HD)
            numer += jnp.dot(
                p.reshape(GRP * n, tokens).astype(BF16), values, preferred_element_type=F32
            )
        peak = peak.reshape(GRP * n, 1)
        total = total.reshape(GRP * n, 1)
        total_hi = total.astype(BF16).astype(F32)
        total_lo = total - total_hi
        stats = jnp.where(
            lane_sq == 0, peak, jnp.where(lane_sq == 1, total_hi, jnp.where(lane_sq == 2, total_lo, 0.0))
        )
        stats = stats.T[:PAD_B].astype(BF16)
        for part in range(per_group):
            to = g * per_group + part
            send_b[to, :chunk, :] = numer[part * chunk : (part + 1) * chunk].astype(BF16)
            send_b[to, chunk : chunk + PAD_B, :] = stats
        for part in range(per_group):
            to = g * per_group + part
            dest = core * dests + to

            @pl.when(dest != me)
            def _():
                at(send_b.at[to], got_b.at[chip], sem_bs.at[to], sem_br.at[chip], dest).start()

            @pl.when(dest == me)
            def _():
                got_b[chip] = send_b[to]

    from_core = me // dests
    for i in range(dests):
        src = 2 * i + from_core

        @pl.when(src != me)
        def _():
            at(send_b.at[0], got_b.at[i], sem_bs.at[0], sem_br.at[i], src).wait_recv()

    tiles = [got_b[i, chunk : chunk + PAD_B, :].astype(F32) for i in range(dests)]
    peaks = jnp.concatenate([t[0:1] for t in tiles], axis=0)
    totals = jnp.concatenate([t[1:2] + t[2:3] for t in tiles], axis=0)
    top = jnp.max(peaks, axis=0, keepdims=True)
    factor = jnp.exp(peaks - top)
    factor = factor / jnp.sum(factor * totals, axis=0, keepdims=True)
    factor = jnp.concatenate([factor, jnp.zeros((GRP * n - dests, GRP * n), F32)], axis=0)
    wgt[...] = factor.T
    my_rows = pl.ds(pl.multiple_of(lax.rem(me, per_group) * chunk, chunk), chunk)
    weights = wgt[my_rows, :]
    mixed = jnp.zeros((chunk, HD), F32)
    for i in range(dests):
        mixed += weights[:, i : i + 1] * got_b[i, :chunk, :].astype(F32)
    feat[core] = jnp.concatenate(
        [mixed[q * n : (q + 1) * n] for q in range(hpd)], axis=1
    ).astype(BF16)
    f_pair = at(feat.at[core], feat.at[core], sem_fs.at[0], sem_fr.at[0], partner)
    f_pair.start()
    w_local.wait()
    w_pair.wait_recv()
    f_pair.wait_recv()

    out_rows = half_cols // HD
    step = 1024
    left, right = feat[0], feat[1]
    for c0 in range(0, half_cols, step):
        part = jnp.dot(left, wbuf[0, :, c0 : c0 + step], preferred_element_type=F32)
        part += jnp.dot(right, wbuf[1, :, c0 : c0 + step], preferred_element_type=F32)
        for j in range(step // HD):
            acc[pl.ds(c0 // HD + j, n, stride=out_rows), :] = part[:, j * HD : (j + 1) * HD]
    for r in range(n):
        send_d[r] = acc[r * out_rows : (r + 1) * out_rows, :].astype(BF16)
    sends_d = []
    for k in order:
        peer = lax.rem(me + k, n)
        copy = at(send_d.at[peer], got_d.at[me], sem_ds.at[k], sem_dr.at[me], peer)
        copy.start()
        sends_d.append(copy)
    got_d[me] = send_d[me]
    for k in reversed(order):
        src = lax.rem(me + n - k, n)
        at(send_d.at[0], got_d.at[src], sem_ds.at[k], sem_dr.at[src], src).wait_recv()
    for part in range(2):
        result = jnp.zeros((out_rows, HD), F32)
        for i in range(n // 2):
            result += got_d[2 * i + part].astype(F32)
        out_ref[part * out_rows : (part + 1) * out_rows, :] = result.astype(BF16)

    for copy in sends_a + sends_d:
        copy.wait_send()
    kv_pair.wait_send()
    w_pair.wait_send()
    f_pair.wait_send()
    for to in range(dests):
        dest = core * dests + to

        @pl.when(dest != me)
        def _():
            at(send_b.at[to], got_b.at[chip], sem_bs.at[to], sem_br.at[chip], dest).wait_send()


def fused(query, kv_pool, holder_table, slot_table, lengths, out_weight):
    n = lax.axis_size("pool")
    slots, _, blk, width = kv_pool.shape
    rows_dev, model = out_weight.shape
    hpd = rows_dev // HD
    rows_a = H // 2 + PAD_A
    out_rows = model // 2 // HD
    chunk = hpd * n
    vmem = pl.BlockSpec(memory_space=pltpu.VMEM)
    hbm = pl.BlockSpec(memory_space=pl.ANY)
    dma = pltpu.SemaphoreType.DMA
    result = pl.pallas_call(
        functools.partial(kernel, n, slots, blk, hpd),
        out_shape=jax.ShapeDtypeStruct((2 * out_rows, HD), BF16),
        in_specs=[pl.BlockSpec(memory_space=pltpu.SMEM), vmem, vmem, vmem, hbm, hbm],
        out_specs=vmem,
        scratch_shapes=[
            pltpu.VMEM((2, rows_a, HD), F32),
            pltpu.VMEM((2, rows_a, HD), BF16),
            pltpu.VMEM((n, rows_a, HD), BF16),
            pltpu.VMEM((n * rows_a, HD), F32),
            pltpu.VMEM((2 * slots, 2 * slots * blk), BF16),
            pltpu.VMEM((2, slots, 2, blk, width // 2), BF16),
            pltpu.VMEM((2, rows_dev, model // 2), BF16),
            pltpu.VMEM((n // 2, chunk + PAD_B, HD), BF16),
            pltpu.VMEM((n // 2, chunk + PAD_B, HD), BF16),
            pltpu.VMEM((GRP * n, GRP * n), F32),
            pltpu.VMEM((2, n, rows_dev), BF16),
            pltpu.VMEM((n * out_rows, HD), F32),
            pltpu.VMEM((n, out_rows, HD), BF16),
            pltpu.VMEM((n, out_rows, HD), BF16),
            dma((n,)), dma((n,)), dma((n // 2,)), dma((n // 2,)), dma((n,)), dma((n,)),
            dma((2,)), dma((2,)), dma((2,)), dma((1,)), dma((1,)),
        ],
        compiler_params=pltpu.CompilerParams(
            collective_id=0, has_side_effects=True, vmem_limit_bytes=48 * 1024 * 1024
        ),
    )(lengths, query, holder_table, slot_table, kv_pool, out_weight)
    return result.reshape(1, model)


lowest = -1e30


def block_partials(query_heads, kv_blocks):
    head_dim = query_heads.shape[-1]
    kv_heads = query_heads.shape[1]
    block_len = kv_blocks.shape[3]
    block_shape = kv_blocks.shape[:2] + (block_len, kv_heads, head_dim)
    key_part = kv_blocks[:, :, 0].reshape(block_shape)
    value_part = kv_blocks[:, :, 1].reshape(block_shape)
    scores = jnp.einsum(
        "agqd,acbgd->acgqb", query_heads, key_part, preferred_element_type=jnp.float32
    )
    scores = scores * (1.0 / math.sqrt(head_dim))
    maxima = jnp.max(scores, axis=-1)
    shifted = jnp.exp(scores - maxima[..., None])
    totals = jnp.sum(shifted, axis=-1)
    outputs = jnp.einsum(
        "acgqb,acbgd->acgqd",
        shifted.astype(jnp.bfloat16),
        value_part,
        preferred_element_type=jnp.float32,
    )
    return (maxima, outputs, totals)


def merge_blocks(maxima, outputs, totals, live_mask, axis_pos):
    peak_score = jnp.max(jnp.where(live_mask, maxima, lowest), axis=axis_pos, keepdims=True)
    factor = jnp.exp(jnp.where(live_mask, maxima - peak_score, lowest))
    numerator = jnp.sum(factor[..., None] * outputs, axis=axis_pos)
    denominator = jnp.sum(factor * totals, axis=axis_pos)
    return (jnp.squeeze(peak_score, axis_pos), numerator, denominator)


def general(query, kv_pool, holder_table, slot_table, lengths, out_weight):
    pool_size = lax.axis_size("pool")
    my_index = lax.axis_index("pool")
    max_blocks = holder_table.shape[1]
    capacity = 2 * max_blocks // pool_size
    groups = H // KVH
    all_holders, all_slots, all_lengths = (
        lax.all_gather(holder_table, "pool", axis=0, tiled=True),
        lax.all_gather(slot_table, "pool", axis=0, tiled=True),
        lax.all_gather(lengths, "pool", axis=0, tiled=True),
    )
    cap_iota = jnp.arange(capacity, dtype=jnp.int32)
    block_iota = jnp.arange(max_blocks, dtype=jnp.int32)
    held_here = all_holders == my_index
    rank_here = jnp.cumsum(held_here.astype(jnp.int32), axis=1) - 1
    pick_hot = held_here[:, None, :] & (rank_here[:, None, :] == cap_iota[None, :, None])
    pick_slot = jnp.sum(jnp.where(pick_hot, all_slots[:, None, :], 0), axis=-1)
    pick_block = jnp.sum(jnp.where(pick_hot, block_iota[None, None, :], 0), axis=-1)
    send_live = jnp.any(pick_hot, axis=-1) & (pick_block < all_lengths[:, None])
    send_blocks = kv_pool[pick_slot]
    all_queries = lax.all_gather(query, "pool", axis=0, tiled=True)
    maxima, outputs, totals = block_partials(
        all_queries.reshape(pool_size, KVH, groups, HD), send_blocks
    )
    part_peak, part_numer, part_denom = merge_blocks(
        maxima, outputs, totals, send_live[:, :, None, None], 1
    )
    got_peak, got_numer, got_denom = (
        lax.all_to_all(
            part_peak.reshape(pool_size, H), "pool", split_axis=0, concat_axis=0, tiled=True
        ),
        lax.all_to_all(
            part_numer.reshape(pool_size, H * HD), "pool", split_axis=0, concat_axis=0, tiled=True
        ),
        lax.all_to_all(
            part_denom.reshape(pool_size, H), "pool", split_axis=0, concat_axis=0, tiled=True
        ),
    )
    peak_score, numerator, denominator = merge_blocks(
        got_peak.reshape(pool_size, KVH, groups),
        got_numer.reshape(pool_size, KVH, groups, HD),
        got_denom.reshape(pool_size, KVH, groups),
        True,
        0,
    )
    attention = (numerator / denominator[..., None]).reshape(1, H * HD).astype(jnp.bfloat16)
    features = lax.all_to_all(attention, "pool", split_axis=1, concat_axis=0, tiled=True)
    return lax.psum_scatter(
        jnp.dot(features, out_weight, preferred_element_type=jnp.float32),
        "pool",
        scatter_dimension=0,
        tiled=True,
    ).astype(jnp.bfloat16)


def per_device(query, kv_pool, holder_table, slot_table, lengths, out_weight):
    n = lax.axis_size("pool")
    rows_dev, model = out_weight.shape
    slots = kv_pool.shape[0]
    fits = (
        n == 16
        and query.shape[0] == 1
        and rows_dev % HD == 0
        and GRP % max(rows_dev // HD, 1) == 0
        and model % 2048 == 0
        and holder_table.shape[1] == HD
        and 2 * slots == HD
        and slots <= 256
    )
    body = fused if fits else general
    return body(query, kv_pool, holder_table, slot_table, lengths, out_weight)


def solution(mesh):
    placed = (
        P(("grp", "pool"), None),
        P(("grp", "pool"), None, None, None),
        P(("grp", "pool"), None),
        P(("grp", "pool"), None),
        P(("grp", "pool")),
        P("pool", None),
    )
    return jax.shard_map(
        per_device, mesh=mesh, in_specs=placed, out_specs=P(("grp", "pool"), None), check_vma=False
    )
```

```python
import functools
import math

import jax
import jax.numpy as jnp
from jax import lax
from jax.experimental import pallas as pl
from jax.experimental.pallas import tpu as pltpu
from jax.sharding import PartitionSpec as P

H = 32
KVH = 4
HD = 128
GRP = H // KVH
LOW = -float(2**100)
PAD_A = 8
PAD_B = 8
F32 = jnp.float32
BF16 = jnp.bfloat16


def kernel(
    n, slots, blk, hpd, parts,
    len_ref, q_hbm, hold_hbm, slot_hbm, kv_ref, w_ref,
    out_ref,
    q_ref, hold_ref, slot_ref, stage, msg_a, got_a, qf, expand, kvbuf, wbuf, send_b, got_b, wgt, acc, send_d, got_d,
    sem_as, sem_ar, sem_bs, sem_br, sem_ds, sem_dr, sem_loc, sem_pair_s, sem_pair_r,
):
    me = lax.axis_index("pool")
    core = lax.rem(me, 2)
    chip = me // 2
    chips = n // 2
    half = n // 2
    my_half = me // half
    partner = me + 1 - 2 * core
    half_heads = H // 2
    half_feat = (KVH // 2) * HD
    model = w_ref.shape[1]
    rows_a = half_heads + PAD_A
    both = 2 * slots
    tokens = slots * blk
    chip_heads = 2 * hpd
    chunk = chip_heads * half
    per_group = GRP // chip_heads
    near = sorted(range(1, n), key=lambda k: min(k, n - k))

    def at(src, dst, ssem, rsem, peer):
        return pltpu.make_async_remote_copy(
            src_ref=src, dst_ref=dst, send_sem=ssem, recv_sem=rsem,
            device_id={"pool": peer}, device_id_type=pl.DeviceIdType.MESH,
        )

    small = [
        pltpu.make_async_copy(src, dst, sem_loc.at[2 + i])
        for i, (src, dst) in enumerate(
            ((q_hbm, q_ref), (hold_hbm, hold_ref), (slot_hbm, slot_ref))
        )
    ]
    for copy in small:
        copy.start()
    barrier = pltpu.get_barrier_semaphore()
    for k in reversed(near):
        pl.semaphore_signal(
            barrier, inc=1, device_id={"pool": lax.rem(me + k, n)},
            device_id_type=pl.DeviceIdType.MESH,
        )
    own_feat = pl.ds(pl.multiple_of(core * half_feat, HD), half_feat)
    other_feat = pl.ds(pl.multiple_of((1 - core) * half_feat, HD), half_feat)
    kv_local = pltpu.make_async_copy(kv_ref.at[:, :, :, own_feat], kvbuf.at[core], sem_loc.at[0])
    w_local = pltpu.make_async_copy(w_ref, wbuf.at[core], sem_loc.at[1])
    kv_local.start()
    w_local.start()
    for copy in small:
        copy.wait()

    maxb = hold_ref.shape[1]
    live = lax.broadcasted_iota(jnp.int32, (1, maxb), 1) < len_ref[0]
    code = jnp.where(live, hold_ref[...] * slots + slot_ref[...], -1)
    code = jnp.broadcast_to(code, (chips, maxb))
    place = lax.broadcasted_iota(jnp.int32, (chips, both), 0) * both + lax.broadcasted_iota(
        jnp.int32, (chips, both), 1
    )
    count = jnp.zeros((chips, both), F32)
    for j in range(maxb):
        count += jnp.where(code[:, j : j + 1] == place, 1.0, 0.0)
    for part in range(2):
        for h in range(half_heads):
            head = part * half_heads + h
            stage[part, h : h + 1, :] = q_ref[:, head * HD : (head + 1) * HD].astype(F32)
    for part in range(2):
        heads = stage[part].astype(BF16)
        for i in range(chips):
            msg_a[2 * i + part, :half_heads, :] = heads
            msg_a[2 * i + part, half_heads:, :] = jnp.broadcast_to(
                count[i : i + 1], (PAD_A, both)
            ).astype(BF16)

    pl.semaphore_wait(barrier, n - 1)

    sends_a = []
    for k in near:
        peer = lax.rem(me + k, n)
        copy = at(msg_a.at[peer], got_a.at[me], sem_as.at[k], sem_ar.at[me], peer)
        copy.start()
        sends_a.append(copy)
    kv_pair = at(kv_ref.at[:, :, :, other_feat], kvbuf.at[core], sem_pair_s.at[0], sem_pair_r.at[0], partner)
    kv_pair.start()
    w_pair = at(w_ref, wbuf.at[core], sem_pair_s.at[1], sem_pair_r.at[1], partner)
    w_pair.start()

    slot_pos = lax.broadcasted_iota(jnp.int32, expand.shape, 0)
    token_pos = lax.broadcasted_iota(jnp.int32, expand.shape, 1)
    expand[...] = jnp.where(token_pos // blk == slot_pos, 1.0, 0.0).astype(BF16)
    got_a[me] = msg_a[me]

    scale = math.log2(math.e) / math.sqrt(HD)
    lane_sq = lax.broadcasted_iota(jnp.int32, (GRP * half, HD), 1)
    for turn in range(2):
        batch = my_half if turn == 0 else 1 - my_half
        first = batch * half
        for r in range(half):
            src = first + r
            if turn == 0:

                @pl.when(src != me)
                def _():
                    at(msg_a.at[0], got_a.at[src], sem_as.at[0], sem_ar.at[src], src).wait_recv()

            else:
                at(msg_a.at[0], got_a.at[src], sem_as.at[0], sem_ar.at[src], src).wait_recv()
            qf[r * rows_a : (r + 1) * rows_a, :] = got_a[src].astype(F32)
        count = qf[pl.ds(half_heads, half, stride=rows_a), :]
        times = jnp.dot(count.astype(BF16), expand[...], preferred_element_type=F32)
        bias = jnp.where(times > 0.0, jnp.log2(times), LOW)
        if turn == 0:
            kv_local.wait()
            kv_pair.wait_recv()
        for g in range(KVH // 2):
            cols = slice(g * HD, (g + 1) * HD)
            heads = jnp.concatenate(
                [qf[pl.ds(g * GRP + q, half, stride=rows_a), :] for q in range(GRP)], axis=0
            ).astype(BF16)
            scores = []
            for d in range(2):
                keys = kvbuf[d, :, 0, :, cols].reshape(tokens, HD)
                s = lax.dot_general(
                    heads, keys, (((1,), (1,)), ((), ())), preferred_element_type=F32
                )
                here = bias[:, d * tokens : (d + 1) * tokens]
                scores.append((s * scale).reshape(GRP, half, tokens) + here[None])
            peak = jnp.maximum(
                jnp.max(scores[0], axis=-1, keepdims=True),
                jnp.max(scores[1], axis=-1, keepdims=True),
            )
            peak = peak.astype(BF16).astype(F32)
            total = jnp.zeros((GRP, half, 1), F32)
            numer = jnp.zeros((GRP * half, HD), F32)
            for d in range(2):
                p = jnp.exp2(scores[d] - peak)
                total += jnp.sum(p, axis=-1, keepdims=True)
                values = kvbuf[d, :, 1, :, cols].reshape(tokens, HD)
                numer += jnp.dot(
                    p.reshape(GRP * half, tokens).astype(BF16), values, preferred_element_type=F32
                )
            peak = peak.reshape(GRP * half, 1)
            total = total.reshape(GRP * half, 1)
            total_hi = total.astype(BF16).astype(F32)
            total_lo = total - total_hi
            stats = jnp.where(
                lane_sq == 0,
                peak,
                jnp.where(lane_sq == 1, total_hi, jnp.where(lane_sq == 2, total_lo, 0.0)),
            )
            stats = jnp.concatenate([stats, jnp.zeros((HD - GRP * half, HD), F32)], axis=0)
            stats = stats.T[:PAD_B].astype(BF16)
            for sub in range(per_group):
                to = (turn * (KVH // 2) + g) * per_group + sub
                send_b[to, :chunk, :] = numer[sub * chunk : (sub + 1) * chunk].astype(BF16)
                send_b[to, chunk:, :] = stats
            for sub in range(per_group):
                to = (turn * (KVH // 2) + g) * per_group + sub
                dest = 2 * (core * (chips // 2) + g * per_group + sub) + batch

                @pl.when(dest != me)
                def _():
                    at(send_b.at[to], got_b.at[chip], sem_bs.at[to], sem_br.at[chip], dest).start()

                @pl.when(dest == me)
                def _():
                    got_b[chip] = send_b[to]

    from_core = chip // (chips // 2)
    for i in range(chips):
        src = 2 * i + from_core

        @pl.when(src != me)
        def _():
            at(send_b.at[0], got_b.at[i], sem_bs.at[0], sem_br.at[i], src).wait_recv()

    tiles = [got_b[i, chunk : chunk + PAD_B, :].astype(F32) for i in range(chips)]
    peaks = jnp.concatenate([t[0:1] for t in tiles], axis=0)
    totals = jnp.concatenate([t[1:2] + t[2:3] for t in tiles], axis=0)
    used = lax.broadcasted_iota(jnp.int32, totals.shape, 1) < GRP * half
    totals = jnp.where(used, totals, 1.0)
    top = jnp.max(peaks, axis=0, keepdims=True)
    factor = jnp.exp2(peaks - top)
    factor = factor / jnp.sum(factor * totals, axis=0, keepdims=True)
    factor = jnp.concatenate([factor, jnp.zeros((HD - chips, HD), F32)], axis=0)
    wgt[...] = factor.T
    my_rows = pl.ds(pl.multiple_of(lax.rem(chip, per_group) * chunk, chunk), chunk)
    weights = wgt[my_rows, :]
    mixed = jnp.zeros((chunk, HD), F32)
    for i in range(chips):
        mixed += weights[:, i : i + 1] * got_b[i, :chunk, :].astype(F32)
    mixed = mixed.astype(BF16).astype(F32)
    sides = [
        jnp.concatenate(
            [mixed[(d * hpd + q) * half : (d * hpd + q + 1) * half] for q in range(hpd)], axis=1
        ).astype(BF16)
        for d in range(2)
    ]

    w_local.wait()
    w_pair.wait_recv()
    cols_part = model // parts
    out_rows = cols_part // HD
    for part in range(parts):
        span = slice(part * cols_part, (part + 1) * cols_part)
        res = jnp.dot(sides[0], wbuf[0, :, span], preferred_element_type=F32)
        res += jnp.dot(sides[1], wbuf[1, :, span], preferred_element_type=F32)
        for j in range(out_rows):
            acc[part, pl.ds(j, half, stride=out_rows), :] = res[:, j * HD : (j + 1) * HD]
        for r in range(half):
            send_d[part, r] = acc[part, r * out_rows : (r + 1) * out_rows, :].astype(BF16)
        for k in range(half):
            r = lax.rem(me + k, half)
            dest = core * half + r

            @pl.when(dest != me)
            def _():
                at(
                    send_d.at[part, r], got_d.at[part, chip], sem_ds.at[part, r],
                    sem_dr.at[part, chip], dest,
                ).start()

            @pl.when(dest == me)
            def _():
                got_d[part, chip] = send_d[part, r]

    for part in range(parts):
        for i in range(chips):
            src = 2 * i + my_half

            @pl.when(src != me)
            def _():
                at(
                    send_d.at[part, 0], got_d.at[part, i], sem_ds.at[part, 0],
                    sem_dr.at[part, i], src,
                ).wait_recv()

        result = jnp.zeros((out_rows, HD), F32)
        for i in range(chips):
            result += got_d[part, i].astype(F32)
        out_ref[part * out_rows : (part + 1) * out_rows, :] = result.astype(BF16)

    for copy in sends_a:
        copy.wait_send()
    kv_pair.wait_send()
    w_pair.wait_send()
    for turn in range(2):
        batch = my_half if turn == 0 else 1 - my_half
        for g in range(KVH // 2):
            for sub in range(per_group):
                to = (turn * (KVH // 2) + g) * per_group + sub
                dest = 2 * (core * (chips // 2) + g * per_group + sub) + batch

                @pl.when(dest != me)
                def _():
                    at(
                        send_b.at[to], got_b.at[chip], sem_bs.at[to], sem_br.at[chip], dest
                    ).wait_send()

    for part in range(parts):
        for r in range(half):
            dest = core * half + r

            @pl.when(dest != me)
            def _():
                at(
                    send_d.at[part, r], got_d.at[part, chip], sem_ds.at[part, r],
                    sem_dr.at[part, chip], dest,
                ).wait_send()


def fused(query, kv_pool, holder_table, slot_table, lengths, out_weight):
    n = lax.axis_size("pool")
    slots, _, blk, width = kv_pool.shape
    rows_dev, model = out_weight.shape
    hpd = rows_dev // HD
    rows_a = H // 2 + PAD_A
    parts = 4
    out_rows = model // parts // HD
    half = n // 2
    chunk = 2 * hpd * half
    vmem = pl.BlockSpec(memory_space=pltpu.VMEM)
    hbm = pl.BlockSpec(memory_space=pltpu.HBM)
    dma = pltpu.SemaphoreType.DMA
    result = pl.pallas_call(
        functools.partial(kernel, n, slots, blk, hpd, parts),
        out_shape=jax.ShapeDtypeStruct((parts * out_rows, HD), BF16),
        in_specs=[pl.BlockSpec(memory_space=pltpu.SMEM)] + [hbm] * 5,
        out_specs=vmem,
        scratch_shapes=[
            pltpu.VMEM(query.shape, BF16),
            pltpu.VMEM(holder_table.shape, jnp.int32),
            pltpu.VMEM(slot_table.shape, jnp.int32),
            pltpu.VMEM((2, H // 2, HD), F32),
            pltpu.VMEM((n, rows_a, HD), BF16),
            pltpu.VMEM((n, rows_a, HD), BF16),
            pltpu.VMEM((half * rows_a, HD), F32),
            pltpu.VMEM((2 * slots, 2 * slots * blk), BF16),
            pltpu.VMEM((2, slots, 2, blk, width // 2), BF16),
            pltpu.VMEM((2, rows_dev, model), BF16),
            pltpu.VMEM((half, chunk + PAD_B, HD), BF16),
            pltpu.VMEM((half, chunk + PAD_B, HD), BF16),
            pltpu.VMEM((HD, HD), F32),
            pltpu.VMEM((parts, half * out_rows, HD), F32),
            pltpu.VMEM((parts, half, out_rows, HD), BF16),
            pltpu.VMEM((parts, half, out_rows, HD), BF16),
            dma((n,)), dma((n,)), dma((half,)), dma((half,)), dma((parts, half)), dma((parts, half)),
            dma((5,)), dma((2,)), dma((2,)),
        ],
        compiler_params=pltpu.CompilerParams(
            collective_id=0, has_side_effects=True, vmem_limit_bytes=67_043_328
        ),
    )(lengths, query, holder_table, slot_table, kv_pool, out_weight)
    return result.reshape(1, model)


lowest = -1e30


def block_partials(query_heads, kv_blocks):
    head_dim = query_heads.shape[-1]
    kv_heads = query_heads.shape[1]
    block_len = kv_blocks.shape[3]
    block_shape = kv_blocks.shape[:2] + (block_len, kv_heads, head_dim)
    key_part = kv_blocks[:, :, 0].reshape(block_shape)
    value_part = kv_blocks[:, :, 1].reshape(block_shape)
    scores = jnp.einsum(
        "agqd,acbgd->acgqb", query_heads, key_part, preferred_element_type=jnp.float32
    )
    scores = scores * (1.0 / math.sqrt(head_dim))
    maxima = jnp.max(scores, axis=-1)
    shifted = jnp.exp(scores - maxima[..., None])
    totals = jnp.sum(shifted, axis=-1)
    outputs = jnp.einsum(
        "acgqb,acbgd->acgqd",
        shifted.astype(jnp.bfloat16),
        value_part,
        preferred_element_type=jnp.float32,
    )
    return (maxima, outputs, totals)


def merge_blocks(maxima, outputs, totals, live_mask, axis_pos):
    peak_score = jnp.max(jnp.where(live_mask, maxima, lowest), axis=axis_pos, keepdims=True)
    factor = jnp.exp(jnp.where(live_mask, maxima - peak_score, lowest))
    numerator = jnp.sum(factor[..., None] * outputs, axis=axis_pos)
    denominator = jnp.sum(factor * totals, axis=axis_pos)
    return (jnp.squeeze(peak_score, axis_pos), numerator, denominator)


def general(query, kv_pool, holder_table, slot_table, lengths, out_weight):
    pool_size = lax.axis_size("pool")
    my_index = lax.axis_index("pool")
    max_blocks = holder_table.shape[1]
    capacity = 2 * max_blocks // pool_size
    groups = H // KVH
    all_holders, all_slots, all_lengths = (
        lax.all_gather(holder_table, "pool", axis=0, tiled=True),
        lax.all_gather(slot_table, "pool", axis=0, tiled=True),
        lax.all_gather(lengths, "pool", axis=0, tiled=True),
    )
    cap_iota = jnp.arange(capacity, dtype=jnp.int32)
    block_iota = jnp.arange(max_blocks, dtype=jnp.int32)
    held_here = all_holders == my_index
    rank_here = jnp.cumsum(held_here.astype(jnp.int32), axis=1) - 1
    pick_hot = held_here[:, None, :] & (rank_here[:, None, :] == cap_iota[None, :, None])
    pick_slot = jnp.sum(jnp.where(pick_hot, all_slots[:, None, :], 0), axis=-1)
    pick_block = jnp.sum(jnp.where(pick_hot, block_iota[None, None, :], 0), axis=-1)
    send_live = jnp.any(pick_hot, axis=-1) & (pick_block < all_lengths[:, None])
    send_blocks = kv_pool[pick_slot]
    all_queries = lax.all_gather(query, "pool", axis=0, tiled=True)
    maxima, outputs, totals = block_partials(
        all_queries.reshape(pool_size, KVH, groups, HD), send_blocks
    )
    part_peak, part_numer, part_denom = merge_blocks(
        maxima, outputs, totals, send_live[:, :, None, None], 1
    )
    got_peak, got_numer, got_denom = (
        lax.all_to_all(
            part_peak.reshape(pool_size, H), "pool", split_axis=0, concat_axis=0, tiled=True
        ),
        lax.all_to_all(
            part_numer.reshape(pool_size, H * HD), "pool", split_axis=0, concat_axis=0, tiled=True
        ),
        lax.all_to_all(
            part_denom.reshape(pool_size, H), "pool", split_axis=0, concat_axis=0, tiled=True
        ),
    )
    peak_score, numerator, denominator = merge_blocks(
        got_peak.reshape(pool_size, KVH, groups),
        got_numer.reshape(pool_size, KVH, groups, HD),
        got_denom.reshape(pool_size, KVH, groups),
        True,
        0,
    )
    attention = (numerator / denominator[..., None]).reshape(1, H * HD).astype(jnp.bfloat16)
    features = lax.all_to_all(attention, "pool", split_axis=1, concat_axis=0, tiled=True)
    return lax.psum_scatter(
        jnp.dot(features, out_weight, preferred_element_type=jnp.float32),
        "pool",
        scatter_dimension=0,
        tiled=True,
    ).astype(jnp.bfloat16)


def per_device(query, kv_pool, holder_table, slot_table, lengths, out_weight):
    n = lax.axis_size("pool")
    rows_dev, model = out_weight.shape
    slots = kv_pool.shape[0]
    fits = (
        n == 16
        and query.shape[0] == 1
        and rows_dev % HD == 0
        and GRP % max(2 * (rows_dev // HD), 1) == 0
        and model % 2048 == 0
        and holder_table.shape[1] == HD
        and 2 * slots == HD
        and KVH % 2 == 0
    )
    body = fused if fits else general
    return body(query, kv_pool, holder_table, slot_table, lengths, out_weight)


def solution(mesh):
    placed = (
        P(("grp", "pool"), None),
        P(("grp", "pool"), None, None, None),
        P(("grp", "pool"), None),
        P(("grp", "pool"), None),
        P(("grp", "pool")),
        P("pool", None),
    )
    return jax.shard_map(
        per_device, mesh=mesh, in_specs=placed, out_specs=P(("grp", "pool"), None), check_vma=False
    )
```

```python
import functools
import math

import jax
import jax.numpy as jnp
from jax import lax
from jax.experimental import pallas as pl
from jax.experimental.pallas import tpu as pltpu
from jax.sharding import PartitionSpec as P

H = 32
KVH = 4
HD = 128
GRP = H // KVH
LOW = -float(2**100)
PAD_A = 8
PAD_B = 8
F32 = jnp.float32
BF16 = jnp.bfloat16


def kernel(
    n, slots, blk, hpd, parts,
    len_ref, q_hbm, hold_hbm, slot_hbm, kv_ref, w_ref,
    out_ref,
    q_ref, hold_ref, slot_ref, stage, msg_a, got_a, qf, expand, kvbuf, keys_t, wbuf, send_b, got_b, wgt, acc, send_d, got_d,
    sem_as, sem_ar, sem_bs, sem_br, sem_ds, sem_dr, sem_loc, sem_pair_s, sem_pair_r,
):
    me = lax.axis_index("pool")
    core = lax.rem(me, 2)
    chip = me // 2
    chips = n // 2
    half = n // 2
    my_half = me // half
    partner = me + 1 - 2 * core
    half_heads = H // 2
    half_feat = (KVH // 2) * HD
    model = w_ref.shape[1]
    rows_a = half_heads + PAD_A
    both = 2 * slots
    tokens = slots * blk
    chip_heads = 2 * hpd
    chunk = chip_heads * half
    per_group = GRP // chip_heads
    near = sorted(range(1, n), key=lambda k: min(k, n - k))

    def at(src, dst, ssem, rsem, peer):
        return pltpu.make_async_remote_copy(
            src_ref=src, dst_ref=dst, send_sem=ssem, recv_sem=rsem,
            device_id={"pool": peer}, device_id_type=pl.DeviceIdType.MESH,
        )

    small = [
        pltpu.make_async_copy(src, dst, sem_loc.at[2 + i])
        for i, (src, dst) in enumerate(
            ((q_hbm, q_ref), (hold_hbm, hold_ref), (slot_hbm, slot_ref))
        )
    ]
    for copy in small:
        copy.start()
    barrier = pltpu.get_barrier_semaphore()
    for k in reversed(near):
        pl.semaphore_signal(
            barrier, inc=1, device_id={"pool": lax.rem(me + k, n)},
            device_id_type=pl.DeviceIdType.MESH,
        )
    own_feat = pl.ds(pl.multiple_of(core * half_feat, HD), half_feat)
    other_feat = pl.ds(pl.multiple_of((1 - core) * half_feat, HD), half_feat)
    kv_local = pltpu.make_async_copy(kv_ref.at[:, :, :, own_feat], kvbuf.at[core], sem_loc.at[0])
    w_local = pltpu.make_async_copy(w_ref, wbuf.at[core], sem_loc.at[1])
    kv_local.start()
    w_local.start()
    for copy in small:
        copy.wait()

    maxb = hold_ref.shape[1]
    live = lax.broadcasted_iota(jnp.int32, (1, maxb), 1) < len_ref[0]
    code = jnp.where(live, hold_ref[...] * slots + slot_ref[...], -1)
    code = jnp.broadcast_to(code, (chips, maxb))
    place = lax.broadcasted_iota(jnp.int32, (chips, both), 0) * both + lax.broadcasted_iota(
        jnp.int32, (chips, both), 1
    )
    count = jnp.zeros((chips, both), F32)
    for j in range(maxb):
        count += jnp.where(code[:, j : j + 1] == place, 1.0, 0.0)
    for part in range(2):
        for h in range(half_heads):
            head = part * half_heads + h
            stage[part, h : h + 1, :] = q_ref[:, head * HD : (head + 1) * HD].astype(F32)
    for part in range(2):
        heads = stage[part].astype(BF16)
        for i in range(chips):
            msg_a[2 * i + part, :half_heads, :] = heads
            msg_a[2 * i + part, half_heads:, :] = jnp.broadcast_to(
                count[i : i + 1], (PAD_A, both)
            ).astype(BF16)

    pl.semaphore_wait(barrier, n - 1)

    sends_a = []
    for k in near:
        peer = lax.rem(me + k, n)
        copy = at(msg_a.at[peer], got_a.at[me], sem_as.at[k], sem_ar.at[me], peer)
        copy.start()
        sends_a.append(copy)
    kv_pair = at(kv_ref.at[:, :, :, other_feat], kvbuf.at[core], sem_pair_s.at[0], sem_pair_r.at[0], partner)
    kv_pair.start()
    w_pair = at(w_ref, wbuf.at[core], sem_pair_s.at[1], sem_pair_r.at[1], partner)
    w_pair.start()

    slot_pos = lax.broadcasted_iota(jnp.int32, expand.shape, 0)
    token_pos = lax.broadcasted_iota(jnp.int32, expand.shape, 1)
    expand[...] = jnp.where(token_pos // blk == slot_pos, 1.0, 0.0).astype(BF16)
    got_a[me] = msg_a[me]

    kv_local.wait()
    kv_pair.wait_recv()
    for g in range(KVH // 2):
        for d in range(2):
            keys = kvbuf[d, :, 0, :, g * HD : (g + 1) * HD].reshape(tokens, HD)
            keys_t[g, :, d * tokens : (d + 1) * tokens] = keys.T

    scale = math.log2(math.e) / math.sqrt(HD)
    lane_sq = lax.broadcasted_iota(jnp.int32, (GRP * half, HD), 1)
    for turn in range(2):
        batch = my_half if turn == 0 else 1 - my_half
        first = batch * half
        for r in range(half):
            src = first + r
            if turn == 0:

                @pl.when(src != me)
                def _():
                    at(msg_a.at[0], got_a.at[src], sem_as.at[0], sem_ar.at[src], src).wait_recv()

            else:
                at(msg_a.at[0], got_a.at[src], sem_as.at[0], sem_ar.at[src], src).wait_recv()
            qf[r * rows_a : (r + 1) * rows_a, :] = got_a[src].astype(F32)
        count = qf[pl.ds(half_heads, half, stride=rows_a), :]
        times = jnp.dot(count.astype(BF16), expand[...], preferred_element_type=F32)
        bias = jnp.where(times > 0.0, jnp.log2(times), LOW)
        for g in range(KVH // 2):
            cols = slice(g * HD, (g + 1) * HD)
            heads = jnp.concatenate(
                [qf[pl.ds(g * GRP + q, half, stride=rows_a), :] for q in range(GRP)], axis=0
            ).astype(BF16)
            scores = []
            for d in range(2):
                keys = keys_t[g, :, d * tokens : (d + 1) * tokens]
                s = jnp.dot(heads, keys, preferred_element_type=F32)
                here = bias[:, d * tokens : (d + 1) * tokens]
                scores.append((s * scale).reshape(GRP, half, tokens) + here[None])
            peak = jnp.maximum(
                jnp.max(scores[0], axis=-1, keepdims=True),
                jnp.max(scores[1], axis=-1, keepdims=True),
            )
            peak = peak.astype(BF16).astype(F32)
            total = jnp.zeros((GRP, half, 1), F32)
            numer = jnp.zeros((GRP * half, HD), F32)
            for d in range(2):
                p = jnp.exp2(scores[d] - peak)
                total += jnp.sum(p, axis=-1, keepdims=True)
                values = kvbuf[d, :, 1, :, cols].reshape(tokens, HD)
                numer += jnp.dot(
                    p.reshape(GRP * half, tokens).astype(BF16), values, preferred_element_type=F32
                )
            peak = peak.reshape(GRP * half, 1)
            total = total.reshape(GRP * half, 1)
            total_hi = total.astype(BF16).astype(F32)
            total_lo = total - total_hi
            stats = jnp.where(
                lane_sq == 0,
                peak,
                jnp.where(lane_sq == 1, total_hi, jnp.where(lane_sq == 2, total_lo, 0.0)),
            )
            stats = jnp.concatenate([stats, jnp.zeros((HD - GRP * half, HD), F32)], axis=0)
            stats = stats.T[:PAD_B].astype(BF16)
            for sub in range(per_group):
                to = (turn * (KVH // 2) + g) * per_group + sub
                send_b[to, :chunk, :] = numer[sub * chunk : (sub + 1) * chunk].astype(BF16)
                send_b[to, chunk:, :] = stats
            for sub in range(per_group):
                to = (turn * (KVH // 2) + g) * per_group + sub
                dest = 2 * (core * (chips // 2) + g * per_group + sub) + batch

                @pl.when(dest != me)
                def _():
                    at(send_b.at[to], got_b.at[chip], sem_bs.at[to], sem_br.at[chip], dest).start()

                @pl.when(dest == me)
                def _():
                    got_b[chip] = send_b[to]

    from_core = chip // (chips // 2)
    for i in range(chips):
        src = 2 * i + from_core

        @pl.when(src != me)
        def _():
            at(send_b.at[0], got_b.at[i], sem_bs.at[0], sem_br.at[i], src).wait_recv()

    tiles = [got_b[i, chunk : chunk + PAD_B, :].astype(F32) for i in range(chips)]
    peaks = jnp.concatenate([t[0:1] for t in tiles], axis=0)
    totals = jnp.concatenate([t[1:2] + t[2:3] for t in tiles], axis=0)
    used = lax.broadcasted_iota(jnp.int32, totals.shape, 1) < GRP * half
    totals = jnp.where(used, totals, 1.0)
    top = jnp.max(peaks, axis=0, keepdims=True)
    factor = jnp.exp2(peaks - top)
    factor = factor / jnp.sum(factor * totals, axis=0, keepdims=True)
    factor = jnp.concatenate([factor, jnp.zeros((HD - chips, HD), F32)], axis=0)
    wgt[...] = factor.T
    my_rows = pl.ds(pl.multiple_of(lax.rem(chip, per_group) * chunk, chunk), chunk)
    weights = wgt[my_rows, :]
    mixed = jnp.zeros((chunk, HD), F32)
    for i in range(chips):
        mixed += weights[:, i : i + 1] * got_b[i, :chunk, :].astype(F32)
    mixed = mixed.astype(BF16).astype(F32)
    sides = [
        jnp.concatenate(
            [mixed[(d * hpd + q) * half : (d * hpd + q + 1) * half] for q in range(hpd)], axis=1
        ).astype(BF16)
        for d in range(2)
    ]

    w_local.wait()
    w_pair.wait_recv()
    cols_part = model // parts
    out_rows = cols_part // HD
    for part in range(parts):
        span = slice(part * cols_part, (part + 1) * cols_part)
        res = jnp.dot(sides[0], wbuf[0, :, span], preferred_element_type=F32)
        res += jnp.dot(sides[1], wbuf[1, :, span], preferred_element_type=F32)
        for j in range(out_rows):
            acc[part, pl.ds(j, half, stride=out_rows), :] = res[:, j * HD : (j + 1) * HD]
        for r in range(half):
            send_d[part, r] = acc[part, r * out_rows : (r + 1) * out_rows, :].astype(BF16)
        for k in range(1, half):
            r = lax.rem(me + k, half)
            at(
                send_d.at[part, r], got_d.at[part, chip], sem_ds.at[part, r],
                sem_dr.at[part, chip], core * half + r,
            ).start()
        mine = lax.rem(me, half)

        @pl.when(core != my_half)
        def _():
            at(
                send_d.at[part, mine], got_d.at[part, chip], sem_ds.at[part, mine],
                sem_dr.at[part, chip], core * half + mine,
            ).start()

        @pl.when(core == my_half)
        def _():
            got_d[part, chip] = send_d[part, mine]

    for part in range(parts):
        for i in range(chips):
            src = 2 * i + my_half

            @pl.when(src != me)
            def _():
                at(
                    send_d.at[part, 0], got_d.at[part, i], sem_ds.at[part, 0],
                    sem_dr.at[part, i], src,
                ).wait_recv()

        result = jnp.zeros((out_rows, HD), F32)
        for i in range(chips):
            result += got_d[part, i].astype(F32)
        out_ref[part * out_rows : (part + 1) * out_rows, :] = result.astype(BF16)

    for copy in sends_a:
        copy.wait_send()
    kv_pair.wait_send()
    w_pair.wait_send()
    for turn in range(2):
        batch = my_half if turn == 0 else 1 - my_half
        for g in range(KVH // 2):
            for sub in range(per_group):
                to = (turn * (KVH // 2) + g) * per_group + sub
                dest = 2 * (core * (chips // 2) + g * per_group + sub) + batch

                @pl.when(dest != me)
                def _():
                    at(
                        send_b.at[to], got_b.at[chip], sem_bs.at[to], sem_br.at[chip], dest
                    ).wait_send()

    for part in range(parts):
        for r in range(half):
            dest = core * half + r

            @pl.when(dest != me)
            def _():
                at(
                    send_d.at[part, r], got_d.at[part, chip], sem_ds.at[part, r],
                    sem_dr.at[part, chip], dest,
                ).wait_send()


def fused(query, kv_pool, holder_table, slot_table, lengths, out_weight):
    n = lax.axis_size("pool")
    slots, _, blk, width = kv_pool.shape
    rows_dev, model = out_weight.shape
    hpd = rows_dev // HD
    rows_a = H // 2 + PAD_A
    parts = 2
    out_rows = model // parts // HD
    half = n // 2
    chunk = 2 * hpd * half
    vmem = pl.BlockSpec(memory_space=pltpu.VMEM)
    hbm = pl.BlockSpec(memory_space=pltpu.HBM)
    dma = pltpu.SemaphoreType.DMA
    result = pl.pallas_call(
        functools.partial(kernel, n, slots, blk, hpd, parts),
        out_shape=jax.ShapeDtypeStruct((parts * out_rows, HD), BF16),
        in_specs=[pl.BlockSpec(memory_space=pltpu.SMEM)] + [hbm] * 5,
        out_specs=vmem,
        scratch_shapes=[
            pltpu.VMEM(query.shape, BF16),
            pltpu.VMEM(holder_table.shape, jnp.int32),
            pltpu.VMEM(slot_table.shape, jnp.int32),
            pltpu.VMEM((2, H // 2, HD), F32),
            pltpu.VMEM((n, rows_a, HD), BF16),
            pltpu.VMEM((n, rows_a, HD), BF16),
            pltpu.VMEM((half * rows_a, HD), F32),
            pltpu.VMEM((2 * slots, 2 * slots * blk), BF16),
            pltpu.VMEM((2, slots, 2, blk, width // 2), BF16),
            pltpu.VMEM((KVH // 2, HD, 2 * slots * blk), BF16),
            pltpu.VMEM((2, rows_dev, model), BF16),
            pltpu.VMEM((half, chunk + PAD_B, HD), BF16),
            pltpu.VMEM((half, chunk + PAD_B, HD), BF16),
            pltpu.VMEM((HD, HD), F32),
            pltpu.VMEM((parts, half * out_rows, HD), F32),
            pltpu.VMEM((parts, half, out_rows, HD), BF16),
            pltpu.VMEM((parts, half, out_rows, HD), BF16),
            dma((n,)), dma((n,)), dma((half,)), dma((half,)), dma((parts, half)), dma((parts, half)),
            dma((5,)), dma((2,)), dma((2,)),
        ],
        compiler_params=pltpu.CompilerParams(
            collective_id=0, has_side_effects=True, vmem_limit_bytes=67_043_328
        ),
    )(lengths, query, holder_table, slot_table, kv_pool, out_weight)
    return result.reshape(1, model)


lowest = -1e30


def block_partials(query_heads, kv_blocks):
    head_dim = query_heads.shape[-1]
    kv_heads = query_heads.shape[1]
    block_len = kv_blocks.shape[3]
    block_shape = kv_blocks.shape[:2] + (block_len, kv_heads, head_dim)
    key_part = kv_blocks[:, :, 0].reshape(block_shape)
    value_part = kv_blocks[:, :, 1].reshape(block_shape)
    scores = jnp.einsum(
        "agqd,acbgd->acgqb", query_heads, key_part, preferred_element_type=jnp.float32
    )
    scores = scores * (1.0 / math.sqrt(head_dim))
    maxima = jnp.max(scores, axis=-1)
    shifted = jnp.exp(scores - maxima[..., None])
    totals = jnp.sum(shifted, axis=-1)
    outputs = jnp.einsum(
        "acgqb,acbgd->acgqd",
        shifted.astype(jnp.bfloat16),
        value_part,
        preferred_element_type=jnp.float32,
    )
    return (maxima, outputs, totals)


def merge_blocks(maxima, outputs, totals, live_mask, axis_pos):
    peak_score = jnp.max(jnp.where(live_mask, maxima, lowest), axis=axis_pos, keepdims=True)
    factor = jnp.exp(jnp.where(live_mask, maxima - peak_score, lowest))
    numerator = jnp.sum(factor[..., None] * outputs, axis=axis_pos)
    denominator = jnp.sum(factor * totals, axis=axis_pos)
    return (jnp.squeeze(peak_score, axis_pos), numerator, denominator)


def general(query, kv_pool, holder_table, slot_table, lengths, out_weight):
    pool_size = lax.axis_size("pool")
    my_index = lax.axis_index("pool")
    max_blocks = holder_table.shape[1]
    capacity = 2 * max_blocks // pool_size
    groups = H // KVH
    all_holders, all_slots, all_lengths = (
        lax.all_gather(holder_table, "pool", axis=0, tiled=True),
        lax.all_gather(slot_table, "pool", axis=0, tiled=True),
        lax.all_gather(lengths, "pool", axis=0, tiled=True),
    )
    cap_iota = jnp.arange(capacity, dtype=jnp.int32)
    block_iota = jnp.arange(max_blocks, dtype=jnp.int32)
    held_here = all_holders == my_index
    rank_here = jnp.cumsum(held_here.astype(jnp.int32), axis=1) - 1
    pick_hot = held_here[:, None, :] & (rank_here[:, None, :] == cap_iota[None, :, None])
    pick_slot = jnp.sum(jnp.where(pick_hot, all_slots[:, None, :], 0), axis=-1)
    pick_block = jnp.sum(jnp.where(pick_hot, block_iota[None, None, :], 0), axis=-1)
    send_live = jnp.any(pick_hot, axis=-1) & (pick_block < all_lengths[:, None])
    send_blocks = kv_pool[pick_slot]
    all_queries = lax.all_gather(query, "pool", axis=0, tiled=True)
    maxima, outputs, totals = block_partials(
        all_queries.reshape(pool_size, KVH, groups, HD), send_blocks
    )
    part_peak, part_numer, part_denom = merge_blocks(
        maxima, outputs, totals, send_live[:, :, None, None], 1
    )
    got_peak, got_numer, got_denom = (
        lax.all_to_all(
            part_peak.reshape(pool_size, H), "pool", split_axis=0, concat_axis=0, tiled=True
        ),
        lax.all_to_all(
            part_numer.reshape(pool_size, H * HD), "pool", split_axis=0, concat_axis=0, tiled=True
        ),
        lax.all_to_all(
            part_denom.reshape(pool_size, H), "pool", split_axis=0, concat_axis=0, tiled=True
        ),
    )
    peak_score, numerator, denominator = merge_blocks(
        got_peak.reshape(pool_size, KVH, groups),
        got_numer.reshape(pool_size, KVH, groups, HD),
        got_denom.reshape(pool_size, KVH, groups),
        True,
        0,
    )
    attention = (numerator / denominator[..., None]).reshape(1, H * HD).astype(jnp.bfloat16)
    features = lax.all_to_all(attention, "pool", split_axis=1, concat_axis=0, tiled=True)
    return lax.psum_scatter(
        jnp.dot(features, out_weight, preferred_element_type=jnp.float32),
        "pool",
        scatter_dimension=0,
        tiled=True,
    ).astype(jnp.bfloat16)


def per_device(query, kv_pool, holder_table, slot_table, lengths, out_weight):
    n = lax.axis_size("pool")
    rows_dev, model = out_weight.shape
    slots = kv_pool.shape[0]
    fits = (
        n == 16
        and query.shape[0] == 1
        and rows_dev % HD == 0
        and GRP % max(2 * (rows_dev // HD), 1) == 0
        and model % 2048 == 0
        and holder_table.shape[1] == HD
        and 2 * slots == HD
        and KVH % 2 == 0
    )
    body = fused if fits else general
    return body(query, kv_pool, holder_table, slot_table, lengths, out_weight)


def solution(mesh):
    placed = (
        P(("grp", "pool"), None),
        P(("grp", "pool"), None, None, None),
        P(("grp", "pool"), None),
        P(("grp", "pool"), None),
        P(("grp", "pool")),
        P("pool", None),
    )
    return jax.shard_map(
        per_device, mesh=mesh, in_specs=placed, out_specs=P(("grp", "pool"), None), check_vma=False
    )
```
